32 devices in a mesh: replica: 8 (over z, y), expert: 4 (over x, core).
Axes of the slice: x: 2, y: 2, z: 4, core: 2. Of those that a mesh axis runs over, the one named last changes fastest.
Arguments:
- local_params: bfloat16 [8, 128, 48, 2048], P('replica', 'expert'), may hold values from -13 to 13, as said below
- base: bfloat16 [128, 48, 2048], P('expert'), may hold values from -6 to 6, as said below
- momentum: float32 [128, 48, 2048], P('expert', None, 'replica'), may hold values from -1.5 to 1.5
- touched: int32 [8, 128], P('replica', 'expert'), may hold values from 0 to 1, as said below
- counts: int32 [8, 128], P('replica', 'expert'), may hold values from 32 to 352, as said below
Outputs:
- new_params: bfloat16 [8, 128, 48, 2048], P('replica', 'expert')
- new_momentum: float32 [128, 48, 2048], P('expert', None, 'replica')
The draws below stay inside these ranges and needn't reach their ends.
Inputs may be any that keep to these rules, and one draw needn't show every extreme that they name: `touched`: among the 32 experts on one device along the `expert` axis, each replica touches at most 16; in every such group some replica touches exactly 16. Positive token counts. `local_params`: Real-valued weights. `base`: Real-valued weights.
All inputs are finite; a program needn't handle non-finite values. Where the reference program divides by a largest or mean magnitude, that divisor is 1e-20 or more.
Results may differ from the reference program's by a relative error of at most 0.0045.
Values may be sent and summed in bfloat16 or wider, within the bound.
No kernel may reach another device: no remote copies, remote signals or barrier semaphores. Data moves between devices by JAX's collectives and lax.ppermute only.
A program may use at most 128 MiB of HBM per device.

```python
import math
import jax
import jax.numpy as jnp
from jax import lax

FF = 2048
EXP_DEV = 32
EXPERTS = 128
ROWS = 48
BLOCK = 128
CAP = 16
REPLICAS = 8


def weight_fields(key):
    key_expert, key_row, key_col, key_base = jax.random.split(jax.random.fold_in(key, 23), 4)
    expert_pos = jnp.arange(EXPERTS, dtype=jnp.float32) / max(EXPERTS - 1, 1)
    col_pos = jnp.arange(FF, dtype=jnp.float32) / max(FF - 1, 1)
    expert_factor = jnp.exp(math.log(3.0) * expert_pos + jax.random.uniform(key_expert, (EXPERTS,), jnp.float32, 0.0, math.log(2.0)))
    row_factor = jnp.exp(jax.random.uniform(key_row, (ROWS,), jnp.float32, 0.0, math.log(10.0)))
    col_factor = jnp.exp(math.log(3.0) * col_pos + jax.random.uniform(key_col, (FF,), jnp.float32, 0.0, math.log(10.0 / 3.0)))
    factors = expert_factor[:, None, None] * row_factor[None, :, None] * col_factor[None, None, :] / 300.0
    base_vals = jnp.clip(jax.random.normal(key_base, (EXPERTS, ROWS, FF), jnp.float32), -3.0, 3.0)
    base_bf = (base_vals * factors).astype(jnp.bfloat16)
    return (base_bf, factors)


def draw_base(key, part):
    base_bf, factors = weight_fields(key)
    return base_bf


def draw_local_params(key, part):
    base_bf, factors = weight_fields(key)
    key_vals = jax.random.fold_in(jax.random.fold_in(key, 41), 0)
    values = jnp.clip(jax.random.normal(key_vals, (REPLICAS, EXPERTS, ROWS, FF), jnp.float32), -4.0, 4.0)
    drift = 0.8 * values
    return (base_bf.astype(jnp.float32)[None] + drift * factors[None]).astype(jnp.bfloat16)


def draw_touched(key, part):
    key_pop, key_noise, key_quota, key_full = jax.random.split(jax.random.fold_in(key, 11), 4)
    groups = EXPERTS // EXP_DEV
    popular = jax.vmap(lambda sub: jax.random.permutation(sub, EXP_DEV))(jax.random.split(key_pop, groups))
    noise = jax.random.randint(key_noise, (REPLICAS, groups, EXP_DEV), 0, EXP_DEV)
    scores = (popular[None] * 2 + noise) * EXP_DEV + popular[None]
    eligible = popular[None] >= EXP_DEV // 8
    scores = jnp.where(eligible, scores, -1 - popular[None])
    ordering = jnp.argsort(-scores, axis=-1)
    ranking = jnp.argsort(ordering, axis=-1)
    quota = jax.random.randint(key_quota, (REPLICAS, groups), max(CAP // 4, 1), CAP + 1)
    full_rep = jax.random.randint(key_full, (groups,), 0, REPLICAS)
    quota = jnp.where(jnp.arange(REPLICAS)[:, None] == full_rep[None, :], CAP, quota)
    chosen = (ranking < quota[:, :, None]) & eligible
    return chosen.reshape(REPLICAS, EXPERTS).astype(jnp.int32)


def draw_counts(key, part):
    key_counts = jax.random.fold_in(key, 31)
    raw_counts = jax.random.randint(key_counts, (REPLICAS, EXPERTS), 32, 129)
    rising = REPLICAS + 2 * jnp.arange(REPLICAS, dtype=jnp.int32)[:, None]
    return (raw_counts * rising // REPLICAS).astype(jnp.int32)


def level_of(key, extent, cuts, least, high):
    loudness, own = 1.0, jax.random.fold_in(key, 6)
    for axis_at, shards_of in cuts:
        steps = jnp.exp(jax.random.uniform(jax.random.fold_in(own, axis_at), (shards_of,), jnp.float32, least / len(cuts), high / len(cuts)))
        loudness = loudness * jnp.repeat(steps, extent[axis_at] // shards_of).reshape([-1 if axis == axis_at else 1 for axis in range(len(extent))])
    return loudness


def normal_values(own_key, dims, spread, limit, cuts=(), held_as=jnp.bfloat16):
    loudness = level_of(own_key, dims, cuts, -0.22, 0.18) if cuts else 1.0
    drawn = jax.random.normal(own_key, dims, jnp.float32) * spread * loudness
    return jnp.minimum(jnp.maximum(drawn, -limit), limit).astype(held_as)


def setup_inputs(seed: int = 0) -> dict:
    key_of = jax.random.split(jax.random.key(seed), 6)
    return {
        "local_params": draw_local_params(jax.random.fold_in(key_of[5], 71), 0),
        "base": draw_base(jax.random.fold_in(key_of[5], 71), 0),
        "momentum": normal_values(key_of[2], (EXPERTS, ROWS, FF), 0.25, 1.5, ((0, 4), (2, 8)), jnp.float32),
        "touched": draw_touched(jax.random.fold_in(key_of[5], 71), 0),
        "counts": draw_counts(jax.random.fold_in(key_of[5], 71), 0),
    }


EPSILON = 1e-06
CLIP_RATIO = 0.02
NESTEROV = 0.9
OUTER_LR = 0.7

def encode(difference):
    leading = difference.shape[:-1]
    blocks = difference.reshape(leading + (difference.shape[-1] // BLOCK, BLOCK))
    block_scale = (lax.optimization_barrier(jnp.max(jnp.abs(blocks), axis=-1)) + EPSILON).astype(jnp.bfloat16)
    code_vals = (blocks / block_scale.astype(jnp.float32)[..., None]).astype(jnp.bfloat16)
    return (code_vals.reshape(difference.shape), block_scale)

def decode(code_vals, block_scale):
    leading = code_vals.shape[:-1]
    blocks = code_vals.astype(jnp.float32).reshape(leading + (block_scale.shape[-1], -1))
    return (blocks * block_scale.astype(jnp.float32)[..., None]).reshape(code_vals.shape)

def reference(local_params, base, momentum, touched, counts):
    weights = (touched * counts).astype(jnp.float32)
    weight_sum = jnp.maximum(lax.optimization_barrier(jnp.sum(weights, axis=0)), 1.0)
    base_wide = base.astype(jnp.float32)

    def add_replica(running, element):
        replica_params, weight_row = element
        code_vals, block_scale = encode(base_wide - replica_params.astype(jnp.float32))
        return (running + weight_row[:, None, None] * decode(code_vals, block_scale), None)
    weighted, _ = lax.scan(add_replica, jnp.zeros(base.shape, jnp.float32), (local_params, weights))
    pseudo = weighted / weight_sum[:, None, None]
    square_sum = jnp.sum(pseudo * pseudo)
    factor = jnp.minimum(1.0, CLIP_RATIO / jnp.sqrt(square_sum / (EXPERTS * ROWS * FF) + EPSILON))
    clipped = factor * pseudo
    new_momentum = NESTEROV * momentum + clipped
    outer_step = -OUTER_LR * (clipped + NESTEROV * new_momentum)
    step_code, step_scale = encode(outer_step)
    renewed = (base_wide + decode(step_code, step_scale)).astype(jnp.bfloat16)
    new_params = jnp.where(touched[:, :, None, None] == 1, renewed[None], local_params)
    return (new_params, new_momentum)
```

```python
import functools

import jax
import jax.numpy as jnp
from jax import lax
from jax.experimental import pallas as pl
from jax.experimental.pallas import tpu as pltpu
from jax.sharding import PartitionSpec as P

CAP = 16
EPSILON = 1e-06
CLIP_RATIO = 0.02
NESTEROV = 0.9
OUTER_LR = 0.7


def slot_table(flags):
    experts = flags.shape[-1]
    e = jnp.arange(experts, dtype=jnp.int32)
    before = (e[:, None] < e[None, :]).astype(jnp.int32)
    rank = jnp.sum(flags[..., :, None] * before, axis=-2)
    slot = jnp.arange(CAP, dtype=jnp.int32)
    hit = (flags[..., None, :] == 1) & (rank[..., None, :] == slot[:, None])
    return jnp.sum(jnp.where(hit, e, 0), axis=-1), rank, jnp.sum(flags, axis=-1)


def butterfly(x, axis, size):
    d = 1
    while d < size:
        x = x + lax.ppermute(x, axis, [(i, i ^ d) for i in range(size)])
        d *= 2
    return x


def pack_kernel(slots, weight, base, params, out, *, owners):
    j = pl.program_id(0)
    w = weight[j].astype(jnp.float32)
    diff = (base[0].astype(jnp.float32) - params[0].astype(jnp.float32)) * w
    wide = diff.shape[1] // owners
    for o in range(owners):
        out[o, 0] = diff[:, o * wide:(o + 1) * wide].astype(jnp.bfloat16)


def reduce_kernel(slot, weight, got, pseudo, square, *, replicas, experts):
    def body(e, acc):
        total = jnp.zeros(pseudo.shape[1:], jnp.float32)
        wsum = jnp.float32(0)
        for r in range(replicas):
            w = weight[r, e].astype(jnp.float32)
            wsum += w
            piece = got[r, jnp.minimum(slot[r, e], CAP - 1)].astype(jnp.float32)
            total += jnp.where(w > 0, piece, 0.0)
        total = total / jnp.full((1, 1), jnp.maximum(wsum, 1.0))
        pseudo[e] = total
        return acc + total * total

    acc = lax.fori_loop(0, experts, body, jnp.zeros(pseudo.shape[1:], jnp.float32))
    square[...] = _fold(acc)


def _fold(acc):
    out = jnp.zeros((8, 128), jnp.float32)
    for i in range(acc.shape[0] // 8):
        for k in range(acc.shape[1] // 128):
            out += acc[i * 8:(i + 1) * 8, k * 128:(k + 1) * 128]
    return out


def step_kernel(slots, square, pseudo, momentum, new_momentum, packed, steps, *, replicas, experts, entries):
    total = jnp.sum(jnp.sum(square[...], axis=0, keepdims=True), axis=1, keepdims=True)
    factor = jnp.minimum(1.0, CLIP_RATIO / jnp.sqrt(total / entries + EPSILON))

    def body(e, _):
        clipped = factor * pseudo[e]
        renewed = NESTEROV * momentum[e] + clipped
        new_momentum[e] = renewed
        steps[e] = (-OUTER_LR * (clipped + NESTEROV * renewed)).astype(jnp.bfloat16)
        return 0

    lax.fori_loop(0, experts, body, 0)

    def fill(j, _):
        for r in range(replicas):
            packed[r, j] = steps[slots[r, j]]
        return 0

    lax.fori_loop(0, CAP, fill, 0)


def keep_kernel(flag, params, out, hold, sem_in, sem_out, *, experts):
    def each(fn):
        def body(e, _):
            pl.when(flag[e] == 0)(lambda: fn(e))
            return 0

        lax.fori_loop(0, experts, body, 0)

    def copy_in(e):
        return pltpu.make_async_copy(params.at[e], hold.at[e], sem_in.at[e])

    def copy_out(e):
        return pltpu.make_async_copy(hold.at[e], out.at[e], sem_out.at[e])

    def turn(e):
        copy_in(e).wait()
        copy_out(e).start()

    each(lambda e: copy_in(e).start())
    each(turn)
    each(lambda e: copy_out(e).wait())


def apply_kernel(slots, count, base, params, step, kept, out, *, owners):
    j = pl.program_id(0)
    wide = base.shape[2] // owners

    @pl.when((j == 0) & (count[0] == 0))
    def _():
        out[0] = params[0]

    @pl.when(j < count[0])
    def _():
        for o in range(owners):
            cols = slice(o * wide, (o + 1) * wide)
            out[0, :, cols] = (base[0, :, cols].astype(jnp.float32) + step[o, 0].astype(jnp.float32)).astype(jnp.bfloat16)


def local(local_params, base, momentum, touched, counts):
    replicas = lax.axis_size("replica")
    shards = lax.axis_size("expert")
    experts, rows, width = base.shape
    wide = width // replicas
    params = local_params[0]
    f32, bf16, i32 = jnp.float32, jnp.bfloat16, jnp.int32
    smem = pl.BlockSpec(memory_space=pltpu.SMEM)
    vmem = pl.BlockSpec(memory_space=pltpu.VMEM)
    hbm = pl.BlockSpec(memory_space=pl.ANY)

    own = lax.axis_index("replica")
    mine = jnp.stack([touched[0], touched[0] * counts[0]])
    place = (jnp.arange(replicas, dtype=i32) == own).astype(i32)
    meta = butterfly(place[:, None, None] * mine, "replica", replicas)

    own_slots, _, own_count = slot_table(touched[0])
    live = jnp.arange(CAP, dtype=i32) < own_count
    last = jnp.max(jnp.where(live, own_slots, 0))
    own_slots = jnp.where(live, own_slots, last)
    own_weight = jnp.where(live, jnp.take(counts[0], own_slots), 0)

    packed = pl.pallas_call(
        functools.partial(pack_kernel, owners=replicas),
        grid_spec=pltpu.PrefetchScalarGridSpec(
            num_scalar_prefetch=2,
            grid=(CAP,),
            in_specs=[pl.BlockSpec((1, rows, width), lambda j, s, w: (s[j], 0, 0))] * 2,
            out_specs=pl.BlockSpec((replicas, 1, rows, wide), lambda j, s, w: (0, j, 0, 0)),
        ),
        out_shape=jax.ShapeDtypeStruct((replicas, CAP, rows, wide), bf16),
        name="pack",
    )(own_slots, own_weight, base, params)

    got = lax.all_to_all(packed, "replica", split_axis=0, concat_axis=0, tiled=True)

    all_slots, all_rank, _ = slot_table(meta[:, 0])
    pseudo, square = pl.pallas_call(
        functools.partial(reduce_kernel, replicas=replicas, experts=experts),
        in_specs=[smem, smem, vmem],
        out_specs=[vmem, vmem],
        out_shape=[jax.ShapeDtypeStruct((experts, rows, wide), f32), jax.ShapeDtypeStruct((8, 128), f32)],
        name="reduce",
    )(all_rank, meta[:, 1], got)

    square = butterfly(butterfly(square, "expert", shards), "replica", replicas)

    new_momentum, packed = pl.pallas_call(
        functools.partial(step_kernel, replicas=replicas, experts=experts, entries=experts * shards * rows * width),
        in_specs=[smem, vmem, vmem, vmem],
        out_specs=[vmem, vmem],
        out_shape=[jax.ShapeDtypeStruct((experts, rows, wide), f32), jax.ShapeDtypeStruct((replicas, CAP, rows, wide), bf16)],
        scratch_shapes=[pltpu.VMEM((experts, rows, wide), bf16)],
        name="step",
    )(all_slots, square, pseudo, momentum)

    got = lax.all_to_all(packed, "replica", split_axis=0, concat_axis=0, tiled=True)

    kept = pl.pallas_call(
        functools.partial(keep_kernel, experts=experts),
        in_specs=[smem, hbm],
        out_specs=hbm,
        out_shape=jax.ShapeDtypeStruct(params.shape, bf16),
        scratch_shapes=[pltpu.VMEM(params.shape, bf16), pltpu.SemaphoreType.DMA((experts,)), pltpu.SemaphoreType.DMA((experts,))],
        name="keep",
    )(touched[0], params)

    new_params = pl.pallas_call(
        functools.partial(apply_kernel, owners=replicas),
        grid_spec=pltpu.PrefetchScalarGridSpec(
            num_scalar_prefetch=2,
            grid=(CAP,),
            in_specs=[
                pl.BlockSpec((1, rows, width), lambda j, s, c: (s[j], 0, 0)),
                pl.BlockSpec((1, rows, width), lambda j, s, c: (s[0], 0, 0)),
                pl.BlockSpec((replicas, 1, rows, wide), lambda j, s, c: (0, j, 0, 0)),
                hbm,
            ],
            out_specs=pl.BlockSpec((1, rows, width), lambda j, s, c: (s[j], 0, 0)),
        ),
        out_shape=jax.ShapeDtypeStruct(params.shape, bf16),
        input_output_aliases={5: 0},
        name="apply",
    )(own_slots, own_count[None], base, params, got, kept)
    return new_params[None], new_momentum


def solution(mesh):
    return jax.shard_map(
        local,
        mesh=mesh,
        in_specs=(
            P("replica", "expert", None, None),
            P("expert", None, None),
            P("expert", None, "replica"),
            P("replica", "expert"),
            P("replica", "expert"),
        ),
        out_specs=(P("replica", "expert", None, None), P("expert", None, "replica")),
        check_vma=False,
    )
```
